256 devices in a mesh: cand: 2 (over core), mp: 64 (over y, x_lo, z), dp: 2 (over x_hi).
Axes of the slice: x: 4 (x_hi: 2, x_lo: 2; x = x_hi * 2 + x_lo), y: 4, z: 8, core: 2. Of those that a mesh axis runs over, the one named last changes fastest.
Arguments:
- clean: bfloat16 [1536, 768], P('mp', 'dp'), may hold values from -3 to 3
- noise: bfloat16 [1536, 768], P('mp', 'dp'), may hold values from -6 to 6
- level_index: int32 [12], P('dp'), may hold values from 0 to 31
- snap_first: bfloat16 [16, 9, 1536, 1536], P('cand', None, 'mp'), may hold values from -0.0546875 to 0.0546875
- snap_second: bfloat16 [16, 9, 1536, 1536], P('cand', None, 'mp'), may hold values from -0.0546875 to 0.0546875
- blend: float32 [4, 8], P('cand'), may hold values from -1.4 to 1.4
- snap_index: int32 [4, 8], P('cand'), may hold values from 0 to 15
Outputs:
- losses: float32 [4], P('cand')
- denoised: bfloat16 [4, 1536, 768], P('cand', 'mp', 'dp')
The draws below stay inside these ranges and needn't reach their ends.
All inputs are finite; a program needn't handle non-finite values.
Results may differ from the reference program's by a relative error of at most 0.00265.
The reference program's roundings to bfloat16 on the way (of `x_in` and `hidden`) count: a program that leaves them out, or rounds other values in their place, can miss the bound.
Values may be sent and summed in bfloat16 or wider, within the bound.
No kernel may reach another device: no remote copies, remote signals or barrier semaphores. Data moves between devices by JAX's collectives and lax.ppermute only.
A program may use at most 128 MiB of HBM per device.

```python
import jax
import jax.numpy as jnp
from jax import lax

C = 1536
CANDS = 4
SNAPS = 16
USE = 8
LEVELS = 32
IMAGES = 12
TOKENS = 768


def plant(array, rng, low, largest):
    shape = array.shape
    spot = [jax.random.randint(jax.random.fold_in(rng, axis), (), 0, shape[axis]) for axis in range(len(shape))]
    array = array.at[tuple(spot)].set(low)
    longest = shape.index(max(shape))
    spot[longest] = (spot[longest] + 1) % shape[longest]
    return array.at[tuple(spot)].set(largest)


def levels(own_key, extent, pieces, low, largest):
    factor_of = 1.0
    for position, parts in pieces:
        heights = jax.random.uniform(jax.random.fold_in(jax.random.fold_in(own_key, 6), position), (parts,), jnp.float32, low / len(pieces), largest / len(pieces))
        factor_of = factor_of * jnp.repeat(jnp.exp(heights), extent[position] // parts).reshape((-1,) + (1,) * (len(extent) - 1 - position))
    return factor_of


def scatter_about(key, shape, scale, reach, split=(), dtype=jnp.bfloat16):
    array = scale * jax.random.normal(key, shape, jnp.float32)
    if split:
        array = array * levels(key, shape, split, -0.22, 0.18)
    return jnp.clip(array, -reach, reach).astype(dtype)


def setup_inputs(seed: int = 0) -> dict:
    splits = jax.random.split(jax.random.key(seed), 8)
    return {
        "clean": scatter_about(splits[0], (C, TOKENS), 0.5, 3.0, ((0, 64), (1, 2))),
        "noise": scatter_about(splits[1], (C, TOKENS), 1.0, 6.0, ((0, 64), (1, 2))),
        "level_index": plant(jax.random.randint(splits[2], (IMAGES,), 0, LEVELS), jax.random.fold_in(splits[2], 1), 0, LEVELS - 1).astype(jnp.int32),
        "snap_first": scatter_about(splits[3], (SNAPS, 9, C, C), (9 * C) ** -0.5, 0.0546875, ((0, 2), (2, 64))),
        "snap_second": scatter_about(splits[4], (SNAPS, 9, C, C), (9 * C) ** -0.5, 0.0546875, ((0, 2), (2, 64))),
        "blend": scatter_about(splits[5], (CANDS, USE), 0.35, 1.4, ((0, 2),), jnp.float32),
        "snap_index": plant(jax.random.randint(splits[6], (CANDS, USE), 0, SNAPS), jax.random.fold_in(splits[6], 1), 0, SNAPS - 1).astype(jnp.int32),
    }


SIGMA_DATA = 0.5

def noise_scale(level_index):
    ratio = 2.0 * level_index.astype(jnp.float32) / (LEVELS - 1) - 1.0
    return jnp.exp(-0.4 + 2.0 * ratio)

def tap_shift(values, down_by, right_by):
    length_all = values.shape[-1]
    offset = down_by * 8 + right_by
    padded = jnp.pad(values, [(0, 0)] * (values.ndim - 1) + [(9, 9)])
    moved = lax.slice_in_dim(padded, 9 + offset, 9 + offset + length_all, axis=values.ndim - 1)
    within = jnp.arange(length_all) % 64
    map_row = within // 8
    map_col = within % 8
    inside = (map_row + down_by >= 0) & (map_row + down_by < 8) & (map_col + right_by >= 0) & (map_col + right_by < 8)
    return jnp.where(inside, moved, jnp.zeros_like(moved))

def tap_stack(values):
    return jnp.stack([tap_shift(values, down_by, right_by) for down_by in (-1, 0, 1) for right_by in (-1, 0, 1)], 0)

def reference(clean, noise, level_index, snap_first, snap_second, blend, snap_index):
    sigmas = jnp.repeat(noise_scale(level_index), 64)
    spread = sigmas * sigmas + SIGMA_DATA * SIGMA_DATA
    scale_in = 1.0 / jnp.sqrt(spread)
    scale_skip = SIGMA_DATA * SIGMA_DATA / spread
    scale_out = sigmas * SIGMA_DATA / jnp.sqrt(spread)
    weighting = spread / (sigmas * SIGMA_DATA) ** 2
    clean_f = clean.astype(jnp.float32)
    noisy = clean_f + sigmas * noise.astype(jnp.float32)
    x_in = (scale_in * noisy).astype(jnp.bfloat16)
    x_stack = tap_stack(x_in).astype(jnp.float32)
    width = clean.shape[0]

    def candidate_loss(member):

        def accumulate(which, totals):
            chosen = snap_index[member, which].astype(jnp.int32)
            coeff = blend[member, which]
            first_snap = lax.dynamic_index_in_dim(snap_first, chosen, 0, keepdims=False).astype(jnp.float32)
            second_snap = lax.dynamic_index_in_dim(snap_second, chosen, 0, keepdims=False).astype(jnp.float32)
            return (totals[0] + coeff * first_snap, totals[1] + coeff * second_snap)
        empty = jnp.zeros((9, width, width), jnp.float32)
        first_w, second_w = lax.fori_loop(0, USE, accumulate, (empty, empty))
        first_w = lax.optimization_barrier(first_w.astype(jnp.bfloat16)).astype(jnp.float32)
        second_w = lax.optimization_barrier(second_w.astype(jnp.bfloat16)).astype(jnp.float32)
        preact = jnp.einsum('koc,kct->ot', first_w, x_stack, precision=lax.Precision.HIGHEST)
        hidden = lax.optimization_barrier(jax.nn.silu(preact).astype(jnp.bfloat16))
        h_stack = tap_stack(hidden).astype(jnp.float32)
        feature = jnp.einsum('kio,kit->ot', second_w, h_stack, precision=lax.Precision.HIGHEST)
        denoised_f = scale_skip * noisy + scale_out * feature
        loss_value = jnp.mean(weighting * (denoised_f - clean_f) ** 2)
        return (loss_value, denoised_f.astype(jnp.bfloat16))
    losses, denoised = lax.map(candidate_loss, jnp.arange(CANDS))
    return (losses, denoised)
```

```python
import jax
import jax.numpy as jnp
from jax import lax
from jax.experimental import pallas as pl
from jax.experimental.pallas import tpu as pltpu
from jax.sharding import Mesh
from jax.sharding import PartitionSpec as P

LEVELS = 32
MP = ("mp_0", "mp_1", "mp_2")


SIGMA_DATA = 0.5


def sent_to_all(value, axis):
    copies = jnp.broadcast_to(value, (lax.axis_size(axis), *value.shape))
    return lax.all_to_all(copies, axis, split_axis=0, concat_axis=0, tiled=True)


def joined_along(pieces, dim):
    pieces = jnp.moveaxis(pieces, 0, dim)
    lengths = pieces.shape
    return pieces.reshape(*lengths[:dim], lengths[dim] * lengths[dim + 1], *lengths[dim + 2 :])


def gathered_copies(value, axis, dim):
    pieces = sent_to_all(value, axis)
    return joined_along(pieces, dim)


def from_partner(value, axis, apart):
    return lax.ppermute(value, axis, [(i, i ^ 1 << apart) for i in range(lax.axis_size(axis))])


def split_up(value, dim, size):
    lengths = value.shape
    pieces = value.reshape(*lengths[:dim], size, lengths[dim] // size, *lengths[dim + 1 :])
    return jnp.moveaxis(pieces, dim, 0)


def sum_at_owner(value, axis, dim):
    pieces = split_up(value, dim, lax.axis_size(axis))
    arrived = lax.all_to_all(pieces, axis, split_axis=0, concat_axis=0, tiled=True)
    return arrived.sum(axis=0)


def summed_rows(value, axes, dim):
    far, near = axes
    initial = sum_at_owner(value, far, dim)
    return sum_at_owner(initial, near, dim)


def over_copies(value, axis):
    return sent_to_all(value, axis).sum(axis=0)


def over_axes(value, axes):
    far, near = axes
    return over_copies(over_copies(value, near), far)


def noise_scale(level_index):
    ratio = 2.0 * level_index.astype(jnp.float32) / (LEVELS - 1) - 1.0
    return jnp.exp(-0.4 + 2.0 * ratio)


def tap_shift(values, down_by, right_by):
    length_all = values.shape[-1]
    offset = down_by * 8 + right_by
    padded = jnp.pad(values, [(0, 0)] * (values.ndim - 1) + [(9, 9)])
    moved = lax.slice_in_dim(padded, 9 + offset, 9 + offset + length_all, axis=values.ndim - 1)
    within = jnp.arange(length_all) % 64
    map_row = within // 8
    map_col = within % 8
    inside = (
        (map_row + down_by >= 0)
        & (map_row + down_by < 8)
        & (map_col + right_by >= 0)
        & (map_col + right_by < 8)
    )
    return jnp.where(inside, moved, jnp.zeros_like(moved))


def tap_stack(values):
    return jnp.stack(
        [tap_shift(values, down_by, right_by) for down_by in (-1, 0, 1) for right_by in (-1, 0, 1)],
        0,
    )


MIB = 1024 * 1024


def blend_kernel(mix_ref, snap_ref, mine_ref, give_ref):
    snaps, _, _, width = snap_ref.shape
    members = mine_ref.shape[0]
    step = 256

    @pl.loop(0, width // step)
    def _(j):
        cols = pl.ds(pl.multiple_of(j * step, step), step)
        totals = [None] * (2 * members)
        for k in range(snaps):
            values = snap_ref[k, 0, :, cols].astype(jnp.float32)
            for row in range(2 * members):
                term = mix_ref[row, k] * values
                totals[row] = term if totals[row] is None else totals[row] + term
        for row in range(members):
            mine_ref[row, 0, :, cols] = totals[row]
            give_ref[row, 0, :, cols] = totals[members + row]


def blend_owned(snap_own, mix_rows):
    snaps, taps, rows, width = snap_own.shape
    members = mix_rows.shape[0] // 2
    out = jax.ShapeDtypeStruct((members, taps, rows, width), jnp.float32)
    spec = pl.BlockSpec((members, 1, rows, width), lambda k: (0, k, 0, 0))
    return pl.pallas_call(
        blend_kernel,
        grid=(taps,),
        out_shape=(out, out),
        in_specs=[
            pl.BlockSpec(memory_space=pltpu.SMEM),
            pl.BlockSpec((snaps, 1, rows, width), lambda k: (0, k, 0, 0)),
        ],
        out_specs=(spec, spec),
        cost_estimate=pl.CostEstimate(
            flops=16 * taps * rows * width * snaps,
            bytes_accessed=2 * snaps * taps * rows * width + 16 * members * taps * rows * width // 2,
            transcendentals=0,
        ),
        name="blend",
    )(mix_rows, snap_own)


def shifted(values, down_by, right_by):
    tokens = values.shape[1]
    offset = down_by * 8 + right_by
    moved = values if offset == 0 else pltpu.roll(values, (-offset) % tokens, 1)
    token = lax.broadcasted_iota(jnp.int32, values.shape, 1)
    row = ((token >> 3) & 7) + down_by
    col = (token & 7) + right_by
    inside = (row >= 0) & (row < 8) & (col >= 0) & (col < 8)
    return jnp.where(inside, moved, 0.0)


TAPS = [(a, b) for a in (-1, 0, 1) for b in (-1, 0, 1)]


def first_kernel(w_ref, x_ref, hidden_ref, acc_ref):
    step = pl.program_id(0)
    part = jnp.dot(w_ref[...], x_ref[...], preferred_element_type=jnp.float32)

    @pl.when(step == 0)
    def _():
        acc_ref[...] = part

    @pl.when(step > 0)
    def _():
        acc_ref[...] += part

    @pl.when(step == pl.num_programs(0) - 1)
    def _():
        members, rows, _ = hidden_ref.shape
        for c in range(members):
            total = None
            for k, (a, b) in enumerate(TAPS):
                start = (c * len(TAPS) + k) * rows
                term = shifted(acc_ref[start : start + rows, :], a, b)
                total = term if total is None else total + term
            hidden_ref[c] = (total * (1.0 / (1.0 + jnp.exp(-total)))).astype(jnp.bfloat16)


def first_layer(w, x):
    members, taps, rows, width = w.shape
    tokens = x.shape[1]
    step = 256
    return pl.pallas_call(
        first_kernel,
        grid=(width // step,),
        out_shape=jax.ShapeDtypeStruct((members, rows, tokens), jnp.bfloat16),
        in_specs=[
            pl.BlockSpec((members * taps * rows, step), lambda i: (0, i)),
            pl.BlockSpec((step, tokens), lambda i: (i, 0)),
        ],
        out_specs=pl.BlockSpec((members, rows, tokens), lambda i: (0, 0, 0)),
        scratch_shapes=[pltpu.VMEM((members * taps * rows, tokens), jnp.float32)],
        cost_estimate=pl.CostEstimate(
            flops=2 * members * taps * rows * width * tokens,
            bytes_accessed=2 * members * taps * rows * width + 2 * width * tokens,
            transcendentals=members * rows * tokens,
        ),
        name="first_layer",
    )(w.reshape(members * taps * rows, width), x)


def on_device(clean, noise, level_index, snap_first, snap_second, blend, snap_index):
    sigmas = jnp.repeat(noise_scale(level_index), 64)
    spread = sigmas * sigmas + SIGMA_DATA * SIGMA_DATA
    scale_in = 1.0 / jnp.sqrt(spread)
    scale_skip = SIGMA_DATA * SIGMA_DATA / spread
    scale_out = sigmas * SIGMA_DATA / jnp.sqrt(spread)
    weighting = spread / (sigmas * SIGMA_DATA) ** 2
    clean_f = clean.astype(jnp.float32)
    noisy = clean_f + sigmas * noise.astype(jnp.float32)
    x_own = (scale_in * noisy).astype(jnp.bfloat16)
    x_full = gathered_copies(x_own, MP, 0)
    owned = snap_first.shape[0]
    stored = owned * lax.axis_size("cand")
    onehot = (snap_index[:, :, None] == jnp.arange(stored, dtype=jnp.int32)[None, None, :]).astype(
        jnp.float32
    )
    mixing = jnp.sum(blend[:, :, None] * onehot, 1)
    first_slot = lax.axis_index("cand") * owned
    other_mix = from_partner(mixing, "cand", 0)
    mix_rows = lax.dynamic_slice_in_dim(
        jnp.concatenate([mixing, other_mix], 0), first_slot, owned, 1
    )
    mine_first, give_first = blend_owned(snap_first, mix_rows)
    got_first = from_partner(give_first, "cand", 0)
    mine_second, give_second = blend_owned(snap_second, mix_rows)
    got_second = from_partner(give_second, "cand", 0)
    first_w = (mine_first + got_first).astype(jnp.bfloat16)
    second_w = (mine_second + got_second).astype(jnp.bfloat16)
    hidden = first_layer(first_w, x_full)
    h_stack = tap_stack(hidden)
    shares = summed_rows(
        jnp.einsum("gkio,kgit->ogt", second_w, h_stack, preferred_element_type=jnp.float32),
        ("mp_0", ("mp_1", "mp_2")),
        0,
    )
    features = jnp.transpose(shares, (1, 0, 2))
    denoised_f = scale_skip[None, None, :] * noisy[None] + scale_out[None, None, :] * features
    partial_value = jnp.sum(
        weighting[None, None, :] * (denoised_f - clean_f[None]) ** 2, axis=(1, 2)
    )
    entries = clean.shape[0] * lax.axis_size(MP) * clean.shape[1] * lax.axis_size("dp")
    totals = over_copies(partial_value, (*MP, "dp"))
    losses = totals / entries
    return (losses, denoised_f.astype(jnp.bfloat16))


def solution(mesh):
    torus = Mesh(
        mesh.devices.reshape(mesh.shape["cand"], 4, 2, 8, mesh.shape["dp"]),
        ("cand", "mp_0", "mp_1", "mp_2", "dp"),
    )
    return jax.shard_map(
        on_device,
        mesh=torus,
        in_specs=(
            P(MP, "dp"),
            P(MP, "dp"),
            P("dp"),
            P("cand", None, MP, None),
            P("cand", None, MP, None),
            P("cand", None),
            P("cand", None),
        ),
        out_specs=(P("cand"), P("cand", MP, "dp")),
        check_vma=False,
    )
```

```python
import jax
import jax.numpy as jnp
from jax import lax
from jax.experimental import pallas as pl
from jax.experimental.pallas import tpu as pltpu
from jax.sharding import Mesh
from jax.sharding import PartitionSpec as P

LEVELS = 32
MP = ("mp_0", "mp_1", "mp_2")
ROWS = ("mp_0", "mp_1")


SIGMA_DATA = 0.5


def sent_to_all(value, axis):
    copies = jnp.broadcast_to(value, (lax.axis_size(axis), *value.shape))
    return lax.all_to_all(copies, axis, split_axis=0, concat_axis=0, tiled=True)


def from_partner(value, axis, apart):
    return lax.ppermute(value, axis, [(i, i ^ 1 << apart) for i in range(lax.axis_size(axis))])


def over_copies(value, axis):
    return sent_to_all(value, axis).sum(axis=0)


def noise_scale(level_index):
    ratio = 2.0 * level_index.astype(jnp.float32) / (LEVELS - 1) - 1.0
    return jnp.exp(-0.4 + 2.0 * ratio)


def weighted_rows(mix_ref, row, values):
    total = None
    for n, value in enumerate(values):
        term = mix_ref[row, n] * value
        total = term if total is None else total + term
    return total


def give_kernel(mix_ref, start_ref, snap_ref, out_ref, own, totals, in_sems, out_sems):
    snaps, chunks, rows, width = own.shape
    step = 256
    start = start_ref[0]

    def arriving(k):
        span = pl.ds(pl.multiple_of(start + k * rows, 8), rows)
        return pltpu.make_async_copy(snap_ref.at[:, span, :], own.at[:, k], in_sems.at[k])

    def leaving(k):
        span = pl.ds(pl.multiple_of(k * rows, 8), rows)
        return pltpu.make_async_copy(totals.at[:, k], out_ref.at[:, span, :], out_sems.at[k])

    for k in range(chunks):
        arriving(k).start()

    @pl.loop(0, chunks)
    def _(k):
        arriving(k).wait()

        @pl.loop(0, width // step)
        def _(j):
            cols = pl.ds(pl.multiple_of(j * step, step), step)
            values = [own[n, k, :, cols].astype(jnp.float32) for n in range(snaps)]
            for row in range(totals.shape[0]):
                totals[row, k, :, cols] = weighted_rows(mix_ref, row, values)

        leaving(k).start()

    @pl.loop(0, chunks)
    def _(k):
        leaving(k).wait()


ANY = pl.BlockSpec(memory_space=pl.ANY)
SCALARS = pl.BlockSpec(memory_space=pltpu.SMEM)


def given_away(mix, snap, start, chunks, rows):
    snaps, _, width = snap.shape
    members = mix.shape[0]
    return pl.pallas_call(
        give_kernel,
        out_shape=jax.ShapeDtypeStruct((members, chunks * rows, width), jnp.float32),
        in_specs=[SCALARS, SCALARS, ANY],
        out_specs=ANY,
        scratch_shapes=[
            pltpu.VMEM((snaps, chunks, rows, width), jnp.bfloat16),
            pltpu.VMEM((members, chunks, rows, width), jnp.float32),
            pltpu.SemaphoreType.DMA((chunks,)),
            pltpu.SemaphoreType.DMA((chunks,)),
        ],
        cost_estimate=pl.CostEstimate(
            flops=2 * members * chunks * rows * width * snaps,
            bytes_accessed=(2 * snaps + 4 * members) * chunks * rows * width,
            transcendentals=0,
        ),
        name="give",
    )(mix, start.reshape(1), snap)


def keep_kernel(mix_ref, snap_ref, got_ref, out_ref, own, got, kept, in_sems, got_sems, out_sems):
    snaps, chunks, rows, width = own.shape
    step = 256

    def span(k):
        return pl.ds(pl.multiple_of(k * rows, 8), rows)

    def arriving(k):
        return pltpu.make_async_copy(snap_ref.at[:, span(k), :], own.at[:, k], in_sems.at[k])

    def partner(k):
        return pltpu.make_async_copy(got_ref.at[:, span(k), :], got.at[:, k], got_sems.at[k])

    def leaving(k):
        return pltpu.make_async_copy(kept.at[:, k], out_ref.at[:, span(k), :], out_sems.at[k])

    for k in range(chunks):
        arriving(k).start()
        partner(k).start()

    @pl.loop(0, chunks)
    def _(k):
        arriving(k).wait()
        partner(k).wait()

        @pl.loop(0, width // step)
        def _(j):
            cols = pl.ds(pl.multiple_of(j * step, step), step)
            values = [own[n, k, :, cols].astype(jnp.float32) for n in range(snaps)]
            for row in range(kept.shape[0]):
                total = weighted_rows(mix_ref, row, values) + got[row, k, :, cols]
                kept[row, k, :, cols] = total.astype(jnp.bfloat16)

        leaving(k).start()

    @pl.loop(0, chunks)
    def _(k):
        leaving(k).wait()


def kept_first(mix, snap, got, chunks):
    snaps, tall, width = snap.shape
    members = mix.shape[0]
    rows = tall // chunks
    return pl.pallas_call(
        keep_kernel,
        out_shape=jax.ShapeDtypeStruct((members, tall, width), jnp.bfloat16),
        in_specs=[SCALARS, ANY, ANY],
        out_specs=ANY,
        scratch_shapes=[
            pltpu.VMEM((snaps, chunks, rows, width), jnp.bfloat16),
            pltpu.VMEM((members, chunks, rows, width), jnp.float32),
            pltpu.VMEM((members, chunks, rows, width), jnp.bfloat16),
            pltpu.SemaphoreType.DMA((chunks,)),
            pltpu.SemaphoreType.DMA((chunks,)),
            pltpu.SemaphoreType.DMA((chunks,)),
        ],
        cost_estimate=pl.CostEstimate(
            flops=2 * members * tall * width * snaps,
            bytes_accessed=(2 * snaps + 6 * members) * tall * width,
            transcendentals=0,
        ),
        name="keep",
    )(mix, snap, got)


def turn_kernel(mix_ref, start_ref, snap_ref, got_ref, out_ref, own, got, turned, in_sems, got_sems, out_sems):
    pieces, snaps, rows, step = own.shape
    members = got.shape[1]
    owners = out_ref.shape[0]
    each = turned.shape[2]
    start = pl.multiple_of(start_ref[0], 8)

    def cols(k):
        return pl.ds(pl.multiple_of(k * step, step), step)

    def arriving(k):
        source = snap_ref.at[:, pl.ds(start, rows), cols(k)]
        return pltpu.make_async_copy(source, own.at[k], in_sems.at[k])

    def partner(k):
        return pltpu.make_async_copy(got_ref.at[:, :, cols(k)], got.at[k], got_sems.at[k])

    def leaving(g):
        target = out_ref.at[g, :, pl.ds(0, each), :]
        return pltpu.make_async_copy(turned.at[g], target, out_sems.at[g])

    for k in range(pieces):
        arriving(k).start()
        partner(k).start()

    @pl.loop(0, pieces)
    def _(k):
        arriving(k).wait()
        partner(k).wait()
        for part in range(step // 128):
            lanes = slice(part * 128, (part + 1) * 128)
            values = [own[k, n, :, lanes].astype(jnp.float32) for n in range(snaps)]
            for row in range(members):
                total = weighted_rows(mix_ref, row, values) + got[k, row, :, lanes]
                turn = total.T.astype(jnp.bfloat16)
                low = part * 128
                for owner in range(2):
                    first, last = max(low, owner * each), min(low + 128, (owner + 1) * each)
                    if first < last:
                        turned[2 * k + owner, row, first - owner * each : last - owner * each, :] = (
                            turn[first - low : last - low]
                        )
        leaving(2 * k).start()
        leaving(2 * k + 1).start()

    @pl.loop(0, owners)
    def _(g):
        leaving(g).wait()


def turned_second(mix, snap, got, start, extra):
    snaps, _, width = snap.shape
    members, rows, _ = got.shape
    pieces, owners, each = 4, 8, width // 8
    return pl.pallas_call(
        turn_kernel,
        out_shape=jax.ShapeDtypeStruct((owners, members, each + extra, rows), jnp.bfloat16),
        in_specs=[SCALARS, SCALARS, ANY, ANY],
        out_specs=ANY,
        scratch_shapes=[
            pltpu.VMEM((pieces, snaps, rows, width // pieces), jnp.bfloat16),
            pltpu.VMEM((pieces, members, rows, width // pieces), jnp.float32),
            pltpu.VMEM((owners, members, each, rows), jnp.bfloat16),
            pltpu.SemaphoreType.DMA((pieces,)),
            pltpu.SemaphoreType.DMA((pieces,)),
            pltpu.SemaphoreType.DMA((owners,)),
        ],
        cost_estimate=pl.CostEstimate(
            flops=2 * members * rows * width * snaps,
            bytes_accessed=(2 * snaps + 6 * members) * rows * width,
            transcendentals=0,
        ),
        name="turn",
    )(mix, start.reshape(1), snap, got)


TAPS = [(a, b) for a in (-1, 0, 1) for b in (-1, 0, 1)]


def shifted(values, down_by, right_by):
    tokens = values.shape[1]
    offset = down_by * 8 + right_by
    moved = values if offset == 0 else pltpu.roll(values, (-offset) % tokens, 1)
    token = lax.broadcasted_iota(jnp.int32, values.shape, 1)
    row = ((token >> 3) & 7) + down_by
    col = (token & 7) + right_by
    inside = (row >= 0) & (row < 8) & (col >= 0) & (col < 8)
    return jnp.where(inside, moved, 0.0)


def first_kernel(w_ref, x_ref, filled_ref, out_ref, acc_ref, hidden_ref, sems):
    acc_ref[...] = jnp.dot(w_ref[...], x_ref[...], preferred_element_type=jnp.float32)
    owners, members = out_ref.shape[:2]
    rows = acc_ref.shape[0] // (members * len(TAPS))
    lanes = hidden_ref.shape[2]
    tall = hidden_ref.shape[1]

    def leaving(g):
        target = out_ref.at[g, :, pl.ds(out_ref.shape[2] - tall, tall), :]
        return pltpu.make_async_copy(hidden_ref, target, sems.at[g])

    for c in range(members):
        total = None
        for k, (a, b) in enumerate(TAPS):
            start = (c * len(TAPS) + k) * rows
            term = shifted(acc_ref[start : start + rows, :], a, b)
            total = term if total is None else total + term
        total = total * (1.0 / (1.0 + jnp.exp(-total)))
        parts = [total[:, j * lanes : (j + 1) * lanes] for j in range(total.shape[1] // lanes)]
        hidden_ref[c] = jnp.concatenate(parts, 0).astype(jnp.bfloat16)
    for g in range(owners):
        leaving(g).start()
    for g in range(owners):
        leaving(g).wait()


def first_layer(w, x, filled):
    tall, width = w.shape
    tokens = x.shape[1]
    owners, members, _, lanes = filled.shape
    rows = tall // (members * len(TAPS))
    extra = rows * tokens // lanes
    whole = pl.BlockSpec(memory_space=pltpu.VMEM)
    return pl.pallas_call(
        first_kernel,
        out_shape=jax.ShapeDtypeStruct(filled.shape, filled.dtype),
        in_specs=[whole, whole, ANY],
        out_specs=ANY,
        input_output_aliases={2: 0},
        scratch_shapes=[
            pltpu.VMEM((tall, tokens), jnp.float32),
            pltpu.VMEM((members, extra, lanes), jnp.bfloat16),
            pltpu.SemaphoreType.DMA((owners,)),
        ],
        cost_estimate=pl.CostEstimate(
            flops=2 * tall * width * tokens,
            bytes_accessed=2 * tall * width + 2 * width * tokens,
            transcendentals=members * rows * tokens,
        ),
        name="first_layer",
    )(w, x, filled)


def second_kernel(got_ref, out_ref, acc_ref):
    sources, halves, _, lanes = got_ref.shape
    owners, _, rows, tokens = out_ref.shape
    each = owners * rows
    cut = lanes
    blank = jnp.zeros((halves * lanes - len(TAPS) * rows, tokens), jnp.float32)
    for half in range(halves):
        total = None
        for s in range(sources):
            parts = [
                got_ref[s, half, each + j * rows : each + (j + 1) * rows, :].astype(jnp.float32)
                for j in range(tokens // lanes)
            ]
            h = jnp.concatenate(parts, 1)
            stack = jnp.concatenate([shifted(h, a, b) for a, b in TAPS], 0)
            stack = jnp.concatenate([stack[:cut], blank, stack[cut:]], 0).astype(jnp.bfloat16)
            w = jnp.concatenate([got_ref[s, 0, :each, :], got_ref[s, 1, :each, :]], 1)
            term = jnp.dot(w, stack, preferred_element_type=jnp.float32)
            total = term if total is None else total + term
        acc_ref[...] = total
        for z in range(owners):
            out_ref[z, half] = acc_ref[z * rows : (z + 1) * rows, :]


def second_layer(got, rows, tokens):
    sources, halves, _, lanes = got.shape
    whole = pl.BlockSpec(memory_space=pltpu.VMEM)
    return pl.pallas_call(
        second_kernel,
        out_shape=jax.ShapeDtypeStruct((8, halves, rows, tokens), jnp.float32),
        in_specs=[whole],
        out_specs=whole,
        scratch_shapes=[pltpu.VMEM((8 * rows, tokens), jnp.float32)],
        cost_estimate=pl.CostEstimate(
            flops=2 * sources * 8 * rows * 256 * 2 * tokens,
            bytes_accessed=2 * got.size + 4 * 16 * rows * tokens,
            transcendentals=0,
        ),
        name="second_layer",
    )(got)


def on_device(clean, noise, level_index, snap_first, snap_second, blend, snap_index):
    side = lax.axis_index("dp").astype(jnp.int32)
    sigmas = jnp.repeat(noise_scale(level_index), 64)
    spread = sigmas * sigmas + SIGMA_DATA * SIGMA_DATA
    scale_in = 1.0 / jnp.sqrt(spread)
    scale_skip = SIGMA_DATA * SIGMA_DATA / spread
    scale_out = sigmas * SIGMA_DATA / jnp.sqrt(spread)
    weighting = spread / (sigmas * SIGMA_DATA) ** 2
    clean_f = clean.astype(jnp.float32)
    noisy = clean_f + sigmas * noise.astype(jnp.float32)
    x_own = (scale_in * noisy).astype(jnp.bfloat16)
    x_full = sent_to_all(x_own, MP).reshape(-1, x_own.shape[1])
    owned = snap_first.shape[0]
    stored = owned * lax.axis_size("cand")
    onehot = (snap_index[:, :, None] == jnp.arange(stored, dtype=jnp.int32)[None, None, :]).astype(
        jnp.float32
    )
    mixing = jnp.sum(blend[:, :, None] * onehot, 1)
    first_slot = lax.axis_index("cand") * owned
    other_mix = from_partner(mixing, "cand", 0)
    mix_rows = lax.dynamic_slice_in_dim(
        jnp.stack([mixing, other_mix], 0), first_slot, owned, 2
    )
    mix_mine, mix_give = mix_rows[0], mix_rows[1]
    taps, rows, width = snap_first.shape[1:]
    tokens = clean.shape[1]
    tall = taps * rows
    snap_first = snap_first.reshape(owned, tall, width)
    snap_second = snap_second.reshape(owned, tall, width)
    start = side * (tall - 128)
    got_second = from_partner(given_away(mix_give, snap_second, start, 8, 16), "cand", 0)
    got_first = from_partner(
        given_away(mix_give, snap_first, jnp.zeros((), jnp.int32), taps, rows), "cand", 0
    )
    turned = turned_second(mix_mine, snap_second, got_second, start, rows * tokens // 128)
    first_w = kept_first(mix_mine, snap_first, got_first, taps)
    sent = first_layer(first_w.reshape(2 * tall, width), x_full, turned)
    arrived = lax.all_to_all(
        sent.reshape(16, *sent.shape[2:]), (*ROWS, "dp"), split_axis=0, concat_axis=0, tiled=True
    ).reshape(sent.shape)
    shares = second_layer(arrived, rows, tokens).reshape(16, rows, tokens)
    shares = lax.all_to_all(shares, ("mp_2", "dp"), split_axis=0, concat_axis=0, tiled=True)
    features = shares.reshape(8, 2, rows, tokens).sum(axis=0)
    denoised_f = scale_skip[None, None, :] * noisy[None] + scale_out[None, None, :] * features
    partial_value = jnp.sum(
        weighting[None, None, :] * (denoised_f - clean_f[None]) ** 2, axis=(1, 2)
    )
    entries = clean.shape[0] * lax.axis_size(MP) * clean.shape[1] * lax.axis_size("dp")
    totals = over_copies(partial_value, (*MP, "dp"))
    losses = totals / entries
    return (losses, denoised_f.astype(jnp.bfloat16))


def solution(mesh):
    torus = Mesh(
        mesh.devices.reshape(mesh.shape["cand"], 4, 2, 8, mesh.shape["dp"]),
        ("cand", "mp_0", "mp_1", "mp_2", "dp"),
    )
    return jax.shard_map(
        on_device,
        mesh=torus,
        in_specs=(
            P(MP, "dp"),
            P(MP, "dp"),
            P("dp"),
            P("cand", None, MP, None),
            P("cand", None, MP, None),
            P("cand", None),
            P("cand", None),
        ),
        out_specs=(P("cand"), P("cand", MP, "dp")),
        check_vma=False,
    )
```

```python
import jax
import jax.numpy as jnp
from jax import lax
from jax.experimental import pallas as pl
from jax.experimental.pallas import tpu as pltpu
from jax.sharding import Mesh
from jax.sharding import PartitionSpec as P


LEVELS = 32
MP = ("mp_0", "mp_1", "mp_2")
ROWS = ("mp_0", "mp_1")


SIGMA_DATA = 0.5


def from_partner(value, axis, apart):
    return lax.ppermute(value, axis, [(i, i ^ 1 << apart) for i in range(lax.axis_size(axis))])


ANY = pl.BlockSpec(memory_space=pl.ANY)
SCALARS = pl.BlockSpec(memory_space=pltpu.SMEM)
WHOLE = pl.BlockSpec(memory_space=pltpu.VMEM)
MIB = 1024 * 1024
SMALL = pltpu.CompilerParams(vmem_limit_bytes=8 * MIB)


def OUT(shape, dtype):
    return pltpu.VMEM(shape, dtype)


def FAR(value):
    return pltpu.with_memory_space_constraint(value, pltpu.HBM)


def IN(value):
    return pltpu.with_memory_space_constraint(value, pltpu.VMEM)


def token_scales(level_ref, shape):
    image = lax.broadcasted_iota(jnp.int32, shape, 1) >> 6
    level = jnp.zeros(shape, jnp.float32)
    for i in range(level_ref.shape[0]):
        level = jnp.where(image == i, level_ref[i].astype(jnp.float32), level)
    ratio = 2.0 * level / (LEVELS - 1) - 1.0
    sigmas = jnp.exp(-0.4 + 2.0 * ratio)
    spread = sigmas * sigmas + SIGMA_DATA * SIGMA_DATA
    return sigmas, spread


def prepare_kernel(level_ref, clean_ref, noise_ref, out_ref):
    sigmas, spread = token_scales(level_ref, clean_ref.shape)
    noisy = clean_ref[...].astype(jnp.float32) + sigmas * noise_ref[...].astype(jnp.float32)
    value = (1.0 / jnp.sqrt(spread) * noisy).astype(jnp.bfloat16)
    for p in range(out_ref.shape[0]):
        out_ref[p] = value


def prepared(level_index, clean, noise, copies):
    rows, tokens = clean.shape
    return pl.pallas_call(
        prepare_kernel,
        out_shape=OUT((copies, rows, tokens), jnp.bfloat16),
        in_specs=[SCALARS, WHOLE, WHOLE],
        out_specs=WHOLE,
        compiler_params=SMALL,
        cost_estimate=pl.CostEstimate(
            flops=20 * rows * tokens,
            bytes_accessed=2 * (copies + 2) * rows * tokens,
            transcendentals=3 * rows * tokens,
        ),
        name="prepare",
    )(level_index, FAR(clean), FAR(noise))


def final_kernel(level_ref, clean_ref, noise_ref, share_ref, out_ref, loss_ref):
    sigmas, spread = token_scales(level_ref, clean_ref.shape)
    clean = clean_ref[...].astype(jnp.float32)
    noisy = clean + sigmas * noise_ref[...].astype(jnp.float32)
    scale_skip = SIGMA_DATA * SIGMA_DATA / spread
    scale_out = sigmas * SIGMA_DATA / jnp.sqrt(spread)
    weighting = spread / ((sigmas * SIGMA_DATA) * (sigmas * SIGMA_DATA))
    lane = lax.broadcasted_iota(jnp.int32, loss_ref.shape, 2)
    losses = jnp.zeros(loss_ref.shape, jnp.float32)
    for c in range(out_ref.shape[0]):
        feature = share_ref[0, c]
        for z in range(1, share_ref.shape[0]):
            feature = feature + share_ref[z, c]
        denoised = scale_skip * noisy + scale_out * feature
        out_ref[c] = denoised.astype(jnp.bfloat16)
        away = denoised - clean
        losses = jnp.where(lane == c, jnp.sum(weighting * (away * away)), losses)
    loss_ref[...] = losses


def finished(level_index, clean, noise, shares, copies):
    rows, tokens = clean.shape
    members = shares.shape[1]
    return pl.pallas_call(
        final_kernel,
        out_shape=(
            jax.ShapeDtypeStruct((members, rows, tokens), jnp.bfloat16),
            OUT((copies, 1, 128), jnp.float32),
        ),
        in_specs=[SCALARS, WHOLE, WHOLE, WHOLE],
        out_specs=(WHOLE, WHOLE),
        compiler_params=SMALL,
        cost_estimate=pl.CostEstimate(
            flops=40 * members * rows * tokens,
            bytes_accessed=4 * shares.size + 8 * rows * tokens,
            transcendentals=3 * rows * tokens,
        ),
        name="final",
    )(level_index, clean, noise, IN(shares))


def weighted_rows(mix_ref, row, values):
    total = None
    for n, value in enumerate(values):
        term = mix_ref[row, n] * value
        total = term if total is None else total + term
    return total


def give_kernel(mix_ref, start_ref, snap_ref, out_ref):
    snaps = snap_ref.shape[0]
    members, tall, width = out_ref.shape
    rows, step = 8, 768
    start = start_ref[0]

    @pl.loop(0, tall // rows)
    def _(k):
        source = pl.ds(pl.multiple_of(start + k * rows, 8), rows)
        target = pl.ds(pl.multiple_of(k * rows, 8), rows)
        for j in range(width // step):
            cols = slice(j * step, (j + 1) * step)
            values = [snap_ref[n, source, cols].astype(jnp.float32) for n in range(snaps)]
            for row in range(members):
                out_ref[row, target, cols] = weighted_rows(mix_ref, row, values)


def given_away(mix, snap, start, tall):
    snaps, _, width = snap.shape
    members = mix.shape[0]
    return pl.pallas_call(
        give_kernel,
        out_shape=OUT((members, tall, width), jnp.float32),
        in_specs=[SCALARS, SCALARS, WHOLE],
        out_specs=WHOLE,
        cost_estimate=pl.CostEstimate(
            flops=2 * members * tall * width * snaps,
            bytes_accessed=(2 * snaps + 4 * members) * tall * width,
            transcendentals=0,
        ),
        compiler_params=SMALL,
        name="give",
    )(mix, start.reshape(1), IN(snap))


def keep_kernel(mix_ref, snap_ref, got_ref, out_ref):
    snaps = snap_ref.shape[0]
    members, tall, width = out_ref.shape
    rows, step = 8, 768

    @pl.loop(0, tall // rows)
    def _(k):
        span = pl.ds(pl.multiple_of(k * rows, 8), rows)
        for j in range(width // step):
            cols = slice(j * step, (j + 1) * step)
            values = [snap_ref[n, span, cols].astype(jnp.float32) for n in range(snaps)]
            for row in range(members):
                total = weighted_rows(mix_ref, row, values) + got_ref[row, span, cols]
                out_ref[row, span, cols] = total.astype(jnp.bfloat16)


def kept_first(mix, snap, got):
    snaps, tall, width = snap.shape
    members = mix.shape[0]
    return pl.pallas_call(
        keep_kernel,
        out_shape=OUT((members, tall, width), jnp.bfloat16),
        in_specs=[SCALARS, WHOLE, WHOLE],
        out_specs=WHOLE,
        cost_estimate=pl.CostEstimate(
            flops=2 * members * tall * width * snaps,
            bytes_accessed=(2 * snaps + 6 * members) * tall * width,
            transcendentals=0,
        ),
        compiler_params=SMALL,
        name="keep",
    )(mix, IN(snap), IN(got))


def turn_kernel(mix_ref, start_ref, snap_ref, got_ref, out_ref):
    snaps = snap_ref.shape[0]
    members, rows, width = got_ref.shape
    owners = out_ref.shape[0]
    each = width // owners
    source = pl.ds(pl.multiple_of(start_ref[0], 8), rows)

    @pl.loop(0, owners // 2)
    def _(k):
        for part in range(2 * each // 128):
            low = part * 128
            cols = pl.ds(pl.multiple_of(k * 2 * each + low, 128), 128)
            values = [snap_ref[n, source, cols].astype(jnp.float32) for n in range(snaps)]
            for row in range(members):
                total = weighted_rows(mix_ref, row, values) + got_ref[row, :, cols]
                turn = total.T.astype(jnp.bfloat16)
                for owner in range(2):
                    first, last = max(low, owner * each), min(low + 128, (owner + 1) * each)
                    if first < last:
                        span = slice(first - owner * each, last - owner * each)
                        out_ref[2 * k + owner, row, span, :] = turn[first - low : last - low]


def turned_second(mix, snap, got, start, extra):
    snaps, _, width = snap.shape
    members, rows, _ = got.shape
    owners = 8
    return pl.pallas_call(
        turn_kernel,
        out_shape=OUT((owners, members, width // owners + extra, rows), jnp.bfloat16),
        in_specs=[SCALARS, SCALARS, WHOLE, WHOLE],
        out_specs=WHOLE,
        cost_estimate=pl.CostEstimate(
            flops=2 * members * rows * width * snaps,
            bytes_accessed=(2 * snaps + 6 * members) * rows * width,
            transcendentals=0,
        ),
        compiler_params=SMALL,
        name="turn",
    )(mix, start.reshape(1), IN(snap), IN(got))


TAPS = [(a, b) for a in (-1, 0, 1) for b in (-1, 0, 1)]


def shifted(values, down_by, right_by):
    tokens = values.shape[1]
    offset = down_by * 8 + right_by
    moved = values if offset == 0 else pltpu.roll(values, (-offset) % tokens, 1)
    token = lax.broadcasted_iota(jnp.int32, values.shape, 1)
    row = ((token >> 3) & 7) + down_by
    col = (token & 7) + right_by
    inside = (row >= 0) & (row < 8) & (col >= 0) & (col < 8)
    return jnp.where(inside, moved, 0.0)


def first_kernel(w_ref, x_ref, filled_ref, out_ref, acc_ref):
    acc_ref[...] = jnp.dot(w_ref[...], x_ref[...], preferred_element_type=jnp.float32)
    owners, members, end, lanes = out_ref.shape
    rows = acc_ref.shape[0] // (members * len(TAPS))
    tokens = acc_ref.shape[1]
    for c in range(members):
        total = None
        for k, (a, b) in enumerate(TAPS):
            start = (c * len(TAPS) + k) * rows
            term = shifted(acc_ref[start : start + rows, :], a, b)
            total = term if total is None else total + term
        total = total * (1.0 / (1.0 + jnp.exp(-total)))
        parts = [total[:, j * lanes : (j + 1) * lanes] for j in range(tokens // lanes)]
        hidden = jnp.concatenate(parts, 0).astype(jnp.bfloat16)
        for g in range(owners):
            out_ref[g, c, end - hidden.shape[0] :, :] = hidden


def first_layer(w, x, filled):
    tall, width = w.shape
    tokens = x.shape[1]
    return pl.pallas_call(
        first_kernel,
        out_shape=OUT(filled.shape, filled.dtype),
        in_specs=[WHOLE, WHOLE, WHOLE],
        out_specs=WHOLE,
        input_output_aliases={2: 0},
        scratch_shapes=[pltpu.VMEM((tall, tokens), jnp.float32)],
        cost_estimate=pl.CostEstimate(
            flops=2 * tall * width * tokens,
            bytes_accessed=2 * tall * width + 2 * width * tokens,
            transcendentals=tall * tokens // len(TAPS),
        ),
        compiler_params=SMALL,
        name="first_layer",
    )(IN(w), IN(x), IN(filled))


def second_kernel(got_ref, out_ref, acc_ref):
    sources, halves, _, lanes = got_ref.shape
    owners, _, rows, tokens = out_ref.shape
    each = owners * rows
    cut = lanes
    blank = jnp.zeros((halves * lanes - len(TAPS) * rows, tokens), jnp.float32)
    for half in range(halves):
        total = None
        for s in range(sources):
            parts = [
                got_ref[s, half, each + j * rows : each + (j + 1) * rows, :].astype(jnp.float32)
                for j in range(tokens // lanes)
            ]
            h = jnp.concatenate(parts, 1)
            stack = jnp.concatenate([shifted(h, a, b) for a, b in TAPS], 0)
            stack = jnp.concatenate([stack[:cut], blank, stack[cut:]], 0).astype(jnp.bfloat16)
            w = jnp.concatenate([got_ref[s, 0, :each, :], got_ref[s, 1, :each, :]], 1)
            term = jnp.dot(w, stack, preferred_element_type=jnp.float32)
            total = term if total is None else total + term
        acc_ref[...] = total
        for z in range(owners):
            out_ref[z, half] = acc_ref[z * rows : (z + 1) * rows, :]


def second_layer(got, rows, tokens):
    sources, halves, _, _ = got.shape
    return pl.pallas_call(
        second_kernel,
        out_shape=OUT((8, halves, rows, tokens), jnp.float32),
        in_specs=[WHOLE],
        out_specs=WHOLE,
        scratch_shapes=[pltpu.VMEM((8 * rows, tokens), jnp.float32)],
        cost_estimate=pl.CostEstimate(
            flops=2 * sources * 8 * rows * 256 * 2 * tokens,
            bytes_accessed=2 * got.size + 4 * 16 * rows * tokens,
            transcendentals=0,
        ),
        compiler_params=SMALL,
        name="second_layer",
    )(IN(got))


def mix_of(blend, snap_index, first, count):
    stored = first + jnp.arange(count, dtype=jnp.int32)
    chosen = (snap_index[:, :, None] == stored[None, None, :]).astype(jnp.float32)
    return jnp.sum(blend[:, :, None] * chosen, 1)


def computed(clean, noise, level_index, snap_first, snap_second, blend, snap_index):
    side = lax.axis_index("dp").astype(jnp.int32)
    owned, taps, rows, width = snap_first.shape
    tokens = clean.shape[1]
    tall = taps * rows
    snap_first = snap_first.reshape(owned, tall, width)
    snap_second = snap_second.reshape(owned, tall, width)
    start = side * (tall - 128)
    group = lax.axis_index("cand")
    mix_mine = mix_of(blend, snap_index, group * owned, owned)
    mix_give = from_partner(mix_of(blend, snap_index, (1 - group) * owned, owned), "cand", 0)
    copies = prepared(level_index, clean, noise, lax.axis_size("mp_2"))
    x_line = lax.all_to_all(copies, "mp_2", split_axis=0, concat_axis=0, tiled=True)
    x_line = x_line.reshape(-1, tokens)
    x_line = jnp.broadcast_to(x_line, (lax.axis_size(ROWS), *x_line.shape))
    x_full = lax.all_to_all(x_line, ROWS, split_axis=0, concat_axis=0, tiled=True)
    x_full = x_full.reshape(-1, tokens)
    give_second = given_away(mix_give, snap_second, start, 128)
    got_second = from_partner(give_second, "cand", 0)
    mix_give, _ = lax.optimization_barrier((mix_give, give_second))
    give_first = given_away(mix_give, snap_first, jnp.zeros((), jnp.int32), tall)
    got_first = from_partner(give_first, "cand", 0)
    mix_mine, _ = lax.optimization_barrier((mix_mine, give_first))
    turned = turned_second(mix_mine, snap_second, got_second, start, rows * tokens // 128)
    mix_mine, turned = lax.optimization_barrier((mix_mine, turned))
    first_w = kept_first(mix_mine, snap_first, got_first)
    sent = first_layer(first_w.reshape(2 * tall, width), x_full, turned)
    arrived = lax.all_to_all(
        sent.reshape(16, *sent.shape[2:]), (*ROWS, "dp"), split_axis=0, concat_axis=0, tiled=True
    ).reshape(sent.shape)
    shares = second_layer(arrived, rows, tokens).reshape(16, rows, tokens)
    shares = lax.all_to_all(shares, ("mp_2", "dp"), split_axis=0, concat_axis=0, tiled=True)
    shares = shares.reshape(8, 2, rows, tokens)
    everyone = (*MP, "dp")
    denoised, partial = finished(level_index, clean, noise, shares, lax.axis_size(everyone))
    partial = lax.all_to_all(partial, everyone, split_axis=0, concat_axis=0, tiled=True)
    entries = clean.shape[0] * lax.axis_size(MP) * tokens * lax.axis_size("dp")
    losses = jnp.sum(partial, axis=(0, 1))[: denoised.shape[0]] / entries
    return (losses, denoised)


def solution(mesh):
    torus = Mesh(
        mesh.devices.reshape(mesh.shape["cand"], 4, 2, 8, mesh.shape["dp"]),
        ("cand", "mp_0", "mp_1", "mp_2", "dp"),
    )
    return jax.shard_map(
        computed,
        mesh=torus,
        in_specs=(
            P(MP, "dp"),
            P(MP, "dp"),
            P("dp"),
            P("cand", None, MP, None),
            P("cand", None, MP, None),
            P("cand", None),
            P("cand", None),
        ),
        out_specs=(P("cand"), P("cand", MP, "dp")),
        check_vma=False,
    )
```
